32 devices in a mesh: gx: 2 (over x), gy: 4 (over z), gz: 4 (over y, core).
Axes of the slice: x: 2, y: 2, z: 4, core: 2. Of those that a mesh axis runs over, the one named last changes fastest.
Arguments:
- fields: float32 [4, 8, 256, 512], P(None, 'gx', 'gy', 'gz'), may hold values from -8 to 8
- volume_code: int32 [8, 256, 512], P('gx', 'gy', 'gz'), may hold values from 65536 to 1048576
- cut_flag: int32 [8, 256, 512], P('gx', 'gy', 'gz'), may hold values 0 or 1
- member_bits: int32 [8, 256, 512], P('gx', 'gy', 'gz'), may hold values from 0 to 134217727
Outputs:
- merged: float32 [4, 8, 256, 512], P(None, 'gx', 'gy', 'gz')
The draws below stay inside these ranges and needn't reach their ends.
All inputs are finite; a program needn't handle non-finite values. No bound on the sum of `cut_flag` on one device may be relied on, other than what follows from the above.
Results may differ from the reference program's by a relative error of at most 0.00015.
Values sent between devices are 32-bit elements; how exact they have to be, the bound alone decides.
No kernel may reach another device: no remote copies, remote signals or barrier semaphores. Data moves between devices by JAX's collectives and lax.ppermute only.
A program may use at most 128 MiB of HBM per device.

```python
import jax
import jax.numpy as jnp

FIELDS = 4
PASSES = 2
NX = 8
NY = 256
NZ = 512


def set_ends(result, stream_key, low, largest):
    extent = result.shape
    index_at = [jax.random.randint(jax.random.fold_in(stream_key, axis), (), 0, extent[axis]) for axis in range(len(extent))]
    result = result.at[tuple(index_at)].set(low)
    longest = extent.index(max(extent))
    index_at[longest] = (index_at[longest] + 1) % extent[longest]
    return result.at[tuple(index_at)].set(largest)


def steps_of(stream_key, shape, cuts, low, largest):
    factor_of, own = 1.0, jax.random.fold_in(stream_key, 6)
    for dim, shards_of in cuts:
        draws = jnp.exp(jax.random.uniform(jax.random.fold_in(own, dim), (shards_of,), jnp.float32, low / len(cuts), largest / len(cuts)))
        factor_of = factor_of * jnp.repeat(draws, shape[dim] // shards_of).reshape([-1 if axis == dim else 1 for axis in range(len(shape))])
    return factor_of


def normal_values(key, shape, spread, bound, pieces=(), kind=jnp.bfloat16):
    values = jax.random.normal(key, shape, jnp.float32) * spread
    if len(pieces) > 0:
        values = steps_of(key, shape, pieces, -0.22, 0.18) * values
    return jnp.clip(values, min=-bound, max=bound).astype(kind)


def setup_inputs(seed: int = 0) -> dict:
    streams_of = jax.random.split(jax.random.key(seed), 5)
    return {
        "fields": normal_values(streams_of[0], (FIELDS, NX, NY, NZ), 1.0, 8.0, ((1, 2), (2, 4), (3, 4)), jnp.float32),
        "volume_code": set_ends(jax.random.randint(streams_of[1], (NX, NY, NZ), 65536, 1048577), jax.random.fold_in(streams_of[1], 1), 65536, 1048576).astype(jnp.int32),
        "cut_flag": set_ends((jax.random.randint(streams_of[2], (NX, NY, NZ), 0, 3) < 1).astype(jnp.int32), jax.random.fold_in(streams_of[2], 1), 0, 1),
        "member_bits": set_ends(jax.random.randint(streams_of[3], (NX, NY, NZ), 0, 134217728), jax.random.fold_in(streams_of[3], 1), 0, 134217727).astype(jnp.int32),
    }


def reference(fields, volume_code, cut_flag, member_bits):
    kappa = volume_code.astype(jnp.float32) / 1048576.0
    active = member_bits * cut_flag
    offsets = []
    for dx in (-1, 0, 1):
        for dy in (-1, 0, 1):
            for dz in (-1, 0, 1):
                offsets.append((dx, dy, dz))
    state = fields
    for step in range(PASSES):
        volume = jnp.zeros_like(kappa)
        mass = jnp.zeros_like(fields)
        count = jnp.zeros_like(kappa)
        weighted = kappa[None] * state
        for index, shift in enumerate(offsets):
            if index == 13:
                member = jnp.ones_like(kappa)
            else:
                member = jnp.bitwise_and(jnp.right_shift(active, index), 1).astype(jnp.float32)
            volume = volume + jnp.roll(member * kappa, shift, axis=(0, 1, 2))
            mass = mass + jnp.roll(member[None] * weighted, shift, axis=(1, 2, 3))
        hat = mass / volume[None]
        total = jnp.zeros_like(fields)
        for index, shift in enumerate(offsets):
            if index == 13:
                member = jnp.ones_like(kappa)
            else:
                member = jnp.bitwise_and(jnp.right_shift(active, index), 1).astype(jnp.float32)
            back = (-shift[0], -shift[1], -shift[2])
            total = total + member[None] * jnp.roll(hat, back, axis=(1, 2, 3))
            count = count + member
        state = total / count[None]
    return state
```

```python
import functools

import jax
import jax.numpy as jnp
from jax import lax
from jax.experimental import pallas as pl
from jax.experimental.pallas import tpu as pltpu
from jax.sharding import PartitionSpec as P

PASSES = 2
HALO = 2 * PASSES
LANES = 128
GROUP = 16
TOP = 8
LOW_BITS = 14

VMEM = pl.BlockSpec(memory_space=pltpu.VMEM)
PARAMS = pltpu.CompilerParams(vmem_limit_bytes=60 * 2**20)


def offsets():
    return [(dx, dy, dz) for dx in (-1, 0, 1) for dy in (-1, 0, 1) for dz in (-1, 0, 1)]


def bit_of(dx, dy, dz):
    return 9 * (dx + 1) + 3 * (dy + 1) + (dz + 1)


def slot_of(dx, dy, dz):
    index = bit_of(dx, dy, dz)
    return index if index < 13 else index - 1


def roll(value, shift):
    shift = shift % LANES
    return value if shift == 0 else pltpu.roll(value, shift, 1)


def ring(axis, step):
    count = lax.axis_size(axis)
    return [(i, (i + step) % count) for i in range(count)]


def pack_kernel(fields, code, flag, bits, ints, zlo, zhi, ylo, yhi):
    count, sx, sy, sz = fields.shape
    lane = lax.broadcasted_iota(jnp.int32, (sy, LANES), 1)
    low_side = jnp.zeros((sy, LANES), jnp.float32)
    high_side = jnp.zeros((sy, LANES), jnp.float32)
    for p in range(sx):
        active = bits[p] * flag[p]
        ints[0, p] = code[p]
        ints[1, p] = active
        planes = [fields[f, p] for f in range(count)]
        planes.append(code[p].astype(jnp.float32))
        planes.append(jnp.bitwise_and(active, 2**LOW_BITS - 1).astype(jnp.float32))
        planes.append(jnp.right_shift(active, LOW_BITS).astype(jnp.float32))
        for a, plane in enumerate(planes):
            row = (a * sx + p) * HALO
            ylo[pl.ds(row, HALO), :] = plane[:HALO]
            yhi[pl.ds(row, HALO), :] = plane[sy - HALO :]
            first = row
            here = (lane >= first) & (lane < first + HALO)
            low_side = jnp.where(here, roll(plane, first), low_side)
            high_side = jnp.where(here, roll(plane, first + HALO), high_side)
    zlo[...] = low_side
    zhi[...] = high_side


def pack(fields, code, flag, bits):
    count, sx, sy, sz = fields.shape
    rows = (count + 3) * sx * HALO
    f32 = jnp.float32
    return pl.pallas_call(
        pack_kernel,
        out_shape=(
            jax.ShapeDtypeStruct((2, sx, sy, sz), jnp.int32),
            jax.ShapeDtypeStruct((sy, LANES), f32),
            jax.ShapeDtypeStruct((sy, LANES), f32),
            jax.ShapeDtypeStruct((rows, LANES), f32),
            jax.ShapeDtypeStruct((rows, LANES), f32),
        ),
        in_specs=[VMEM] * 4,
        out_specs=(VMEM,) * 5,
        compiler_params=PARAMS,
        name="pack",
    )(fields, code, flag, bits)


class Box:
    def __init__(self, count, sx, sy, blocks):
        self.count, self.sx, self.sy, self.blocks = count, sx, sy, blocks
        self.planes = sx * blocks
        self.tiles = -(-self.planes * GROUP // LANES)
        self.rows = sy + 2 * TOP
        self.steps = -(-(sy + 2 * HALO) // 8)

    def near(self, reach):
        wanted = range(-reach, self.sx + reach)
        return sorted({x % self.planes for x in wanted})


def lane_index():
    return lax.broadcasted_iota(jnp.int32, (8, LANES), 1)


def fill(box, main_of, low_of, high_of, main, strip):
    lane = lane_index()

    def step(t, _):
        r = t * 8 + TOP - HALO
        out = [jnp.zeros((8, LANES), jnp.float32) for _ in range(box.tiles)]
        for b in range(box.blocks):
            lows, highs = low_of(b, r), high_of(b, r)
            for p in range(box.sx):
                x = b * box.sx + p
                tile, first = divmod(x * GROUP, LANES)
                plane = main_of(x, r)
                for c, value in (
                    (0, lows[p]),
                    (HALO, (plane, 0)),
                    (2 * HALO, (plane, LANES - HALO)),
                    (3 * HALO, highs[p]),
                ):
                    data, lane0 = value
                    at = first + c
                    here = (lane >= at) & (lane < at + HALO)
                    out[tile] = jnp.where(here, roll(data, at - lane0), out[tile])
        for tile in range(box.tiles):
            strip[tile, pl.ds(r, 8), :] = out[tile].astype(strip.dtype)
        return 0

    lax.fori_loop(0, box.steps, step, 0)


def roll_groups(values, shift):
    count = len(values)
    rolled = [roll(v, shift) for v in values]
    if count == 1 or shift == 0:
        return rolled
    lane = lane_index()
    if shift > 0:
        return [jnp.where(lane < shift, rolled[(k - 1) % count], rolled[k]) for k in range(count)]
    return [jnp.where(lane >= LANES + shift, rolled[(k + 1) % count], rolled[k]) for k in range(count)]


def add(left, right):
    return right if left is None else left + right


def strip_scatter(box, masks, value, r):
    parts = {}
    for dz in (-1, 0, 1):
        total = [None] * box.tiles
        for dx in (-1, 0, 1):
            sums = [None] * box.tiles
            for dy in (-1, 0, 1):
                for k in range(box.tiles):
                    piece = value[k, pl.ds(r - dy, 8), :]
                    if (dx, dy, dz) != (0, 0, 0):
                        piece = piece * masks[slot_of(dx, dy, dz), k, pl.ds(r - dy, 8), :]
                    sums[k] = add(sums[k], piece)
            sums = roll_groups(sums, GROUP * dx)
            total = [add(t, s) for t, s in zip(total, sums)]
        parts[dz] = total
    up = roll_groups(parts[1], 1)
    down = roll_groups(parts[-1], -1)
    return parts, [a + b + c for a, b, c in zip(parts[0], up, down)]


def from_strip(tiles, x, column, lane):
    tile, first = divmod(x * GROUP + column, LANES)
    return roll(tiles[tile], lane - first)


LAST = HALO - 1
NEXT = 3 * HALO


def main_scatter(box, masks, value, xs, r, parts):
    lane = lane_index()
    count = len(value)
    result = [[None] * len(xs) for _ in range(count)]
    for dz in (0, 1, -1):
        sums = [[None] * len(xs) for _ in range(count)]
        for dy in (-1, 0, 1):
            cells = {}
            for dx in (-1, 0, 1):
                for i, x in enumerate(xs):
                    source = (x - dx) % box.planes
                    if source not in cells:
                        cells[source] = [value[f][source, pl.ds(r - dy, 8), :] for f in range(count)]
                    mask = None
                    if (dx, dy, dz) != (0, 0, 0):
                        mask = masks[slot_of(dx, dy, dz), source, pl.ds(r - dy, 8), :]
                    for f in range(count):
                        piece = cells[source][f]
                        sums[f][i] = add(sums[f][i], piece if mask is None else piece * mask)
        for f in range(count):
            for i, x in enumerate(xs):
                piece = sums[f][i]
                if dz == 1:
                    piece = jnp.where(lane == 0, from_strip(parts[f][1], x, LAST, 0), roll(piece, 1))
                elif dz == -1:
                    piece = jnp.where(lane == LANES - 1, from_strip(parts[f][-1], x, NEXT, LANES - 1), roll(piece, -1))
                result[f][i] = add(result[f][i], piece)
    return result


def main_gather(box, masks, value, xs, r):
    count = len(value)
    sums = [[None] * len(xs) for _ in range(count)]
    for dz in (-1, 0, 1):
        for dy in (-1, 0, 1):
            cells = {}
            for dx in (-1, 0, 1):
                for i, x in enumerate(xs):
                    source = (x + dx) % box.planes
                    if source not in cells:
                        cells[source] = [value[f][dz + 1, source, pl.ds(r + dy, 8), :] for f in range(count)]
                    mask = None
                    if (dx, dy, dz) != (0, 0, 0):
                        mask = masks[slot_of(dx, dy, dz), x, pl.ds(r, 8), :]
                    for f in range(count):
                        piece = cells[source][f]
                        sums[f][i] = add(sums[f][i], piece if mask is None else piece * mask)
    return sums


def chunks(xs, size=4):
    return [xs[i : i + size] for i in range(0, len(xs), size)]


def scatter_stage(box, refs, group, xs):
    masks, smasks, inverse, sinverse = refs["mask"], refs["smask"], refs["inv"], refs["sinv"]
    lane = lane_index()

    def step(t, _):
        r = t * 8 + TOP - HALO
        parts, shats = [], []
        for f in group:
            part, totals = strip_scatter(box, smasks, refs["sw"].at[f], r)
            shat = [total * sinverse[k, pl.ds(r, 8), :] for k, total in enumerate(totals)]
            parts.append(part)
            shats.append(shat)
            for dx in (-1, 0, 1):
                for dz in (-1, 0, 1):
                    shifted = roll_groups(roll_groups(shat, -GROUP * dx), -dz)
                    for k in range(box.tiles):
                        refs["shat"][f, 3 * (dx + 1) + dz + 1, k, pl.ds(r, 8), :] = shifted[k]
        for part_xs in chunks(xs):
            totals = main_scatter(box, masks, [refs["w"].at[f] for f in group], part_xs, r, parts)
            for g, f in enumerate(group):
                for i, x in enumerate(part_xs):
                    hat = totals[g][i] * inverse[x, pl.ds(r, 8), :]
                    refs["hat"][f, 1, x, pl.ds(r, 8), :] = hat
                    refs["hat"][f, 0, x, pl.ds(r, 8), :] = jnp.where(
                        lane == 0, from_strip(shats[g], x, LAST, 0), roll(hat, 1)
                    )
                    refs["hat"][f, 2, x, pl.ds(r, 8), :] = jnp.where(
                        lane == LANES - 1, from_strip(shats[g], x, NEXT, LANES - 1), roll(hat, -1)
                    )
        return 0

    lax.fori_loop(0, box.steps, step, 0)


def gather_stage(box, refs, group, xs, out):
    masks, smasks = refs["mask"], refs["smask"]
    first = TOP - HALO if out is None else TOP
    steps = box.steps if out is None else box.sy // 8

    def step(t, _):
        r = t * 8 + first
        for f in group if out is None else ():
            sums = [None] * box.tiles
            for dx, dy, dz in offsets():
                for k in range(box.tiles):
                    piece = refs["shat"][f, 3 * (dx + 1) + dz + 1, k, pl.ds(r + dy, 8), :]
                    if (dx, dy, dz) != (0, 0, 0):
                        piece = piece * smasks[slot_of(dx, dy, dz), k, pl.ds(r, 8), :]
                    sums[k] = add(sums[k], piece)
            for k in range(box.tiles):
                refs["sw"][f, k, pl.ds(r, 8), :] = sums[k] * refs["sscale"][k, pl.ds(r, 8), :]
        for part_xs in chunks(xs):
            sums = main_gather(box, masks, [refs["hat"].at[f] for f in group], part_xs, r)
            for g, f in enumerate(group):
                for i, x in enumerate(part_xs):
                    if out is None:
                        refs["w"][f, x, pl.ds(r, 8), :] = sums[g][i] * refs["scale"][x, pl.ds(r, 8), :]
                    else:
                        out[f, x, pl.ds(t * 8, 8), :] = sums[g][i] * refs["icount"][x, pl.ds(r, 8), :]
        return 0

    lax.fori_loop(0, steps, step, 0)


def masks_stage(box, refs):
    def one(active, kappa, mask, inv_count, scale, index, r):
        count = None
        for dx, dy, dz in offsets():
            if (dx, dy, dz) == (0, 0, 0):
                continue
            bit = jnp.bitwise_and(jnp.right_shift(active, bit_of(dx, dy, dz)), 1).astype(jnp.float32)
            mask[slot_of(dx, dy, dz), index, pl.ds(r, 8), :] = bit
            count = add(count, bit)
        inverse = 1.0 / (count + 1.0)
        if inv_count is not None:
            inv_count[index, pl.ds(r, 8), :] = inverse
        scale[index, pl.ds(r, 8), :] = inverse * kappa

    def step(t, _):
        r = t * 8 + TOP - HALO
        for k in range(box.tiles):
            kappa = refs["skappa"][k, pl.ds(r, 8), :]
            one(refs["sactive"][k, pl.ds(r, 8), :], kappa, refs["smask"], None, refs["sscale"], k, r)
        for x in range(box.planes):
            kappa = refs["kappa"][x, pl.ds(r, 8), :]
            one(refs["active"][x, pl.ds(r, 8), :], kappa, refs["mask"], refs["icount"], refs["scale"], x, r)
        return 0

    lax.fori_loop(0, box.steps, step, 0)


def volume_stage(box, refs, xs):
    def step(t, _):
        r = t * 8 + TOP - HALO
        part, totals = strip_scatter(box, refs["smask"], refs["skappa"], r)
        for k in range(box.tiles):
            refs["sinv"][k, pl.ds(r, 8), :] = 1.0 / totals[k]
        for part_xs in chunks(xs):
            totals = main_scatter(box, refs["mask"], [refs["kappa"]], part_xs, r, [part])
            for i, x in enumerate(part_xs):
                refs["inv"][x, pl.ds(r, 8), :] = 1.0 / totals[0][i]
        return 0

    lax.fori_loop(0, box.steps, step, 0)


SCRATCH = ("mask", "smask", "inv", "sinv", "w", "sw", "hat", "shat", "icount", "scale", "sscale", "kappa", "skappa", "active", "sactive", "half", "shalf", "zbuf")


def scratch_shapes(box):
    p, k, r, n = box.planes, box.tiles, box.rows, box.count
    f32 = jnp.float32
    return [
        pltpu.VMEM((26, p, r, LANES), f32),
        pltpu.VMEM((26, k, r, LANES), f32),
        pltpu.VMEM((p, r, LANES), f32),
        pltpu.VMEM((k, r, LANES), f32),
        pltpu.VMEM((n, p, r, LANES), f32),
        pltpu.VMEM((n, k, r, LANES), f32),
        pltpu.VMEM((n, 3, p, r, LANES), f32),
        pltpu.VMEM((n, 9, k, r, LANES), f32),
        pltpu.VMEM((p, r, LANES), f32),
        pltpu.VMEM((p, r, LANES), f32),
        pltpu.VMEM((k, r, LANES), f32),
        pltpu.VMEM((p, r, LANES), f32),
        pltpu.VMEM((k, r, LANES), f32),
        pltpu.VMEM((p, r, LANES), jnp.int32),
        pltpu.VMEM((k, r, LANES), jnp.int32),
        pltpu.VMEM((2, p, r, LANES), f32),
        pltpu.VMEM((2, k, r, LANES), f32),
        pltpu.VMEM((2, box.blocks, r, LANES), f32),
    ]


def local_kernel(box, *refs):
    nb, sx, sy, count = box.blocks, box.sx, box.sy, box.count
    fields, refs = refs[:nb], refs[nb:]
    ints, refs = refs[:nb], refs[nb:]
    edges, refs = refs[:nb], refs[nb:]
    out, refs = refs[0], dict(zip(SCRATCH, refs[1:]))
    ymain = (count + 3) * sx * HALO
    ylow, yhigh = 2 * sy, 2 * sy + ymain + 2 * HALO
    own_rows, before, after = pl.ds(TOP, sy), pl.ds(TOP - HALO, HALO), pl.ds(TOP + sy, HALO)
    zbuf = refs["zbuf"]
    for b in range(nb):
        for side in range(2):
            zbuf[side, b, own_rows, :] = edges[b][pl.ds(side * sy, sy), :]
            zbuf[side, b, before, :] = edges[b][pl.ds(ylow + ymain + side * HALO, HALO), :]
            zbuf[side, b, after, :] = edges[b][pl.ds(yhigh + ymain + side * HALO, HALO), :]

    def halo_rows(target, a, x):
        b, p = divmod(x, sx)
        row = (a * sx + p) * HALO
        target[x, before, :] = edges[b][pl.ds(ylow + row, HALO), :]
        target[x, after, :] = edges[b][pl.ds(yhigh + row, HALO), :]

    def strips(a, main, strip):
        def side_of(side):
            def get(b, r):
                tile = zbuf[side, b, pl.ds(r, 8), :]
                return [(tile, (a * sx + p) * HALO) for p in range(sx)]

            return get

        fill(box, lambda x, r: main[x, pl.ds(r, 8), :], side_of(0), side_of(1), main, strip)

    half, shalf = refs["half"], refs["shalf"]
    for x in range(box.planes):
        b, p = divmod(x, sx)
        refs["kappa"][x, own_rows, :] = ints[b][0, p].astype(jnp.float32)
        active = ints[b][1, p]
        half[0, x, own_rows, :] = jnp.bitwise_and(active, 2**LOW_BITS - 1).astype(jnp.float32)
        half[1, x, own_rows, :] = jnp.right_shift(active, LOW_BITS).astype(jnp.float32)
        halo_rows(refs["kappa"], count, x)
        halo_rows(half.at[0], count + 1, x)
        halo_rows(half.at[1], count + 2, x)
    strips(count, refs["kappa"], refs["skappa"])
    for i in range(2):
        strips(count + 1 + i, half.at[i], shalf.at[i])

    def convert(t, _):
        rows = pl.ds(t * 8 + TOP - HALO, 8)
        for full, kappa, active, n in (
            (half, refs["kappa"], refs["active"], box.planes),
            (shalf, refs["skappa"], refs["sactive"], box.tiles),
        ):
            for x in range(n):
                kappa[x, rows, :] = kappa[x, rows, :] * 2.0**-20
                active[x, rows, :] = full[0, x, rows, :].astype(jnp.int32) + full[1, x, rows, :].astype(jnp.int32) * 2**LOW_BITS
        return 0

    lax.fori_loop(0, box.steps, convert, 0)
    masks_stage(box, refs)
    volume_stage(box, refs, box.near(HALO - 1))

    for f in range(count):
        w = refs["w"].at[f]
        for x in range(box.planes):
            b, p = divmod(x, sx)
            w[x, own_rows, :] = fields[b][f, p]
            halo_rows(w, f, x)
        strips(f, w, refs["sw"].at[f])

        def weigh(t, _, f=f):
            rows = pl.ds(t * 8 + TOP - HALO, 8)
            for x in range(box.planes):
                refs["w"][f, x, rows, :] = refs["w"][f, x, rows, :] * refs["kappa"][x, rows, :]
            for k in range(box.tiles):
                refs["sw"][f, k, rows, :] = refs["sw"][f, k, rows, :] * refs["skappa"][k, rows, :]
            return 0

        lax.fori_loop(0, box.steps, weigh, 0)

    for group in chunks(list(range(count)), 2):
        for step in range(PASSES):
            reach = HALO - 1 - 2 * step
            scatter_stage(box, refs, group, box.near(reach))
            gather_stage(box, refs, group, box.near(reach - 1), None if step < PASSES - 1 else out)


def local(box, fields, ints, edges):
    shape = fields[0].shape
    return pl.pallas_call(
        functools.partial(local_kernel, box),
        out_shape=jax.ShapeDtypeStruct(shape, jnp.float32),
        in_specs=[VMEM] * (3 * box.blocks),
        out_specs=VMEM,
        scratch_shapes=scratch_shapes(box),
        compiler_params=PARAMS,
        name="local",
    )(*fields, *ints, *edges)


def body(fields, volume_code, cut_flag, member_bits):
    count, sx, sy, sz = fields.shape
    size = lax.axis_size("gx")

    def from_x(value):
        if size == 1:
            return []
        if size == 2:
            return [lax.ppermute(value, "gx", ring("gx", 1))]
        return [lax.ppermute(value, "gx", ring("gx", -1)), lax.ppermute(value, "gx", ring("gx", 1))]

    ints, zlo, zhi, ylo, yhi = pack(fields, volume_code, cut_flag, member_bits)
    all_fields = [fields] + from_x(fields)
    all_ints = [ints] + from_x(ints)
    low = lax.ppermute(zhi, "gz", ring("gz", 1))
    high = lax.ppermute(zlo, "gz", ring("gz", -1))
    ylo = jnp.concatenate([ylo, low[:HALO], high[:HALO]])
    yhi = jnp.concatenate([yhi, low[sy - HALO :], high[sy - HALO :]])
    before = lax.ppermute(yhi, "gy", ring("gy", 1))
    after = lax.ppermute(ylo, "gy", ring("gy", -1))
    edge = jnp.concatenate([low, high, before, after])
    all_edges = [edge] + from_x(edge)
    box = Box(count, sx, sy, len(all_fields))
    return local(box, all_fields, all_ints, all_edges)


def solution(mesh):
    in_specs = (
        P(None, "gx", "gy", "gz"),
        P("gx", "gy", "gz"),
        P("gx", "gy", "gz"),
        P("gx", "gy", "gz"),
    )
    out_specs = P(None, "gx", "gy", "gz")
    return jax.shard_map(body, mesh=mesh, in_specs=in_specs, out_specs=out_specs, check_vma=False)
```

```python
import functools

import jax
import jax.numpy as jnp
from jax import lax
from jax.experimental import pallas as pl
from jax.experimental.pallas import tpu as pltpu
from jax.sharding import PartitionSpec as P


PASSES = 2
HALO = 2 * PASSES
LANES = 128
GROUP = 16
TOP = 8
LOW_BITS = 14

VMEM = pl.BlockSpec(memory_space=pltpu.VMEM)
ANY = pl.BlockSpec(memory_space=pl.ANY)


def params(mib):
    return pltpu.CompilerParams(vmem_limit_bytes=mib * 2**20)


def offsets():
    return [(dx, dy, dz) for dx in (-1, 0, 1) for dy in (-1, 0, 1) for dz in (-1, 0, 1)]


def bit_of(dx, dy, dz):
    return 9 * (dx + 1) + 3 * (dy + 1) + (dz + 1)


def slot_of(dx, dy, dz):
    index = bit_of(dx, dy, dz)
    return index if index < 13 else index - 1


def roll(value, shift):
    shift = shift % LANES
    return value if shift == 0 else pltpu.roll(value, shift, 1)


def ring(axis, step):
    count = lax.axis_size(axis)
    return [(i, (i + step) % count) for i in range(count)]


def pack_kernel(fields, code, flag, bits, ints, zlo, zhi, ylo, yhi):
    count, sx, sy, _ = fields.shape
    lane = lax.broadcasted_iota(jnp.int32, (sy, LANES), 1)
    low_side = jnp.zeros((sy, LANES), jnp.float32)
    high_side = jnp.zeros((sy, LANES), jnp.float32)
    for p in range(sx):
        active = bits[p] * flag[p]
        ints[0, p] = code[p]
        ints[1, p] = active
        planes = [fields[f, p] for f in range(count)]
        planes.append(code[p].astype(jnp.float32))
        planes.append(jnp.bitwise_and(active, 2**LOW_BITS - 1).astype(jnp.float32))
        planes.append(jnp.right_shift(active, LOW_BITS).astype(jnp.float32))
        for a, plane in enumerate(planes):
            row = (a * sx + p) * HALO
            ylo[pl.ds(row, HALO), :] = plane[:HALO]
            yhi[pl.ds(row, HALO), :] = plane[sy - HALO :]
            first = row
            here = (lane >= first) & (lane < first + HALO)
            low_side = jnp.where(here, roll(plane, first), low_side)
            high_side = jnp.where(here, roll(plane, first + HALO), high_side)
    zlo[...] = low_side
    zhi[...] = high_side


def pack(fields, code, flag, bits):
    count, sx, sy, sz = fields.shape
    rows = (count + 3) * sx * HALO + 2 * HALO
    f32 = jnp.float32
    return pl.pallas_call(
        pack_kernel,
        out_shape=(
            jax.ShapeDtypeStruct((2, sx, sy, sz), jnp.int32),
            jax.ShapeDtypeStruct((sy, LANES), f32),
            jax.ShapeDtypeStruct((sy, LANES), f32),
            jax.ShapeDtypeStruct((rows, LANES), f32),
            jax.ShapeDtypeStruct((rows, LANES), f32),
        ),
        in_specs=[VMEM] * 4,
        out_specs=(VMEM,) * 5,
        compiler_params=params(8),
        name="pack",
    )(fields, code, flag, bits)


def corners_kernel(sy, low, high, ylo_in, yhi_in, ylo, yhi):
    first = ylo.shape[0] - 2 * HALO
    for side, column in enumerate((low, high)):
        rows = pl.ds(first + side * HALO, HALO)
        ylo[rows, :] = column[:HALO]
        yhi[rows, :] = column[sy - HALO :]


def add_corners(low, high, ylo, yhi):
    shape = jax.ShapeDtypeStruct(ylo.shape, ylo.dtype)
    return pl.pallas_call(
        functools.partial(corners_kernel, low.shape[0]),
        out_shape=(shape, shape),
        in_specs=[VMEM] * 4,
        out_specs=(VMEM, VMEM),
        input_output_aliases={2: 0, 3: 1},
        compiler_params=params(2),
        name="corners",
    )(low, high, ylo, yhi)


def join_kernel(*refs):
    out, row = refs[-1], 0
    for ref in refs[:-1]:
        out[pl.ds(row, ref.shape[0]), :] = ref[...]
        row += ref.shape[0]


def join(*pieces):
    rows = sum(piece.shape[0] for piece in pieces)
    return pl.pallas_call(
        join_kernel,
        out_shape=jax.ShapeDtypeStruct((rows, LANES), jnp.float32),
        in_specs=[VMEM] * len(pieces),
        out_specs=VMEM,
        compiler_params=params(2),
        name="join",
    )(*pieces)


class Box:
    def __init__(self, count, sx, sy, blocks):
        self.count, self.sx, self.sy, self.blocks = count, sx, sy, blocks
        self.planes = sx * blocks
        self.tiles = -(-self.planes * GROUP // LANES)
        self.rows = sy + 3 * TOP
        self.steps = -(-(sy + 2 * HALO) // 8)

    def near(self, reach):
        wanted = range(-reach, self.sx + reach)
        return sorted({x % self.planes for x in wanted})


def lane_index():
    return lax.broadcasted_iota(jnp.int32, (8, LANES), 1)


def fill(box, main_of, low_of, high_of, strip):
    lane = lane_index()

    def step(t, _):
        r = t * 8 + TOP - HALO
        out = [jnp.zeros((8, LANES), jnp.float32) for _ in range(box.tiles)]
        for b in range(box.blocks):
            lows, highs = low_of(b, r), high_of(b, r)
            for p in range(box.sx):
                x = b * box.sx + p
                tile, first = divmod(x * GROUP, LANES)
                plane = main_of(x, r)
                for c, value in (
                    (0, lows[p]),
                    (HALO, (plane, 0)),
                    (2 * HALO, (plane, LANES - HALO)),
                    (3 * HALO, highs[p]),
                ):
                    data, lane0 = value
                    at = first + c
                    here = (lane >= at) & (lane < at + HALO)
                    out[tile] = jnp.where(here, roll(data, at - lane0), out[tile])
        for tile in range(box.tiles):
            strip[tile, pl.ds(r, 8), :] = out[tile].astype(strip.dtype)
        return 0

    lax.fori_loop(0, box.steps, step, 0)


def roll_groups(values, shift):
    count = len(values)
    rolled = [roll(v, shift) for v in values]
    if count == 1 or shift == 0:
        return rolled
    lane = lane_index()
    if shift > 0:
        return [jnp.where(lane < shift, rolled[(k - 1) % count], rolled[k]) for k in range(count)]
    return [jnp.where(lane >= LANES + shift, rolled[(k + 1) % count], rolled[k]) for k in range(count)]


def add(left, right):
    return right if left is None else left + right


def strip_scatter(box, masks, value, r):
    parts = {}
    for dz in (-1, 0, 1):
        total = [None] * box.tiles
        for dx in (-1, 0, 1):
            sums = [None] * box.tiles
            for dy in (-1, 0, 1):
                for k in range(box.tiles):
                    piece = value[k, pl.ds(r - dy, 8), :]
                    if (dx, dy, dz) != (0, 0, 0):
                        piece = piece * masks[slot_of(dx, dy, dz), k, pl.ds(r - dy, 8), :]
                    sums[k] = add(sums[k], piece)
            sums = roll_groups(sums, GROUP * dx)
            total = [add(t, s) for t, s in zip(total, sums)]
        parts[dz] = total
    up = roll_groups(parts[1], 1)
    down = roll_groups(parts[-1], -1)
    return parts, [a + b + c for a, b, c in zip(parts[0], up, down)]


def from_strip(tiles, x, column, lane):
    tile, first = divmod(x * GROUP + column, LANES)
    return roll(tiles[tile], lane - first)


LAST = HALO - 1
NEXT = 3 * HALO


def main_scatter(box, masks, value, xs, r, parts):
    lane = lane_index()
    count = len(value)
    result = [[None] * len(xs) for _ in range(count)]
    for dz in (0, 1, -1):
        sums = [[None] * len(xs) for _ in range(count)]
        for dy in (-1, 0, 1):
            cells = {}
            for dx in (-1, 0, 1):
                for i, x in enumerate(xs):
                    source = (x - dx) % box.planes
                    if source not in cells:
                        cells[source] = [value[f][source, pl.ds(r - dy, 8), :] for f in range(count)]
                    mask = None
                    if (dx, dy, dz) != (0, 0, 0):
                        mask = masks[slot_of(dx, dy, dz), source, pl.ds(r - dy, 8), :]
                    for f in range(count):
                        piece = cells[source][f]
                        sums[f][i] = add(sums[f][i], piece if mask is None else piece * mask)
        for f in range(count):
            for i, x in enumerate(xs):
                piece = sums[f][i]
                if dz == 1:
                    piece = jnp.where(lane == 0, from_strip(parts[f][1], x, LAST, 0), roll(piece, 1))
                elif dz == -1:
                    piece = jnp.where(lane == LANES - 1, from_strip(parts[f][-1], x, NEXT, LANES - 1), roll(piece, -1))
                result[f][i] = add(result[f][i], piece)
    return result


def main_gather(box, masks, value, xs, r):
    count = len(value)
    sums = [[None] * len(xs) for _ in range(count)]
    for dz in (-1, 0, 1):
        for dy in (-1, 0, 1):
            cells = {}
            for dx in (-1, 0, 1):
                for i, x in enumerate(xs):
                    source = (x + dx) % box.planes
                    if source not in cells:
                        cells[source] = [value[f][dz + 1, source, pl.ds(r + dy, 8), :] for f in range(count)]
                    mask = None
                    if (dx, dy, dz) != (0, 0, 0):
                        mask = masks[slot_of(dx, dy, dz), x, pl.ds(r, 8), :]
                    for f in range(count):
                        piece = cells[source][f]
                        sums[f][i] = add(sums[f][i], piece if mask is None else piece * mask)
    return sums


def chunks(xs, size=4):
    return [xs[i : i + size] for i in range(0, len(xs), size)]


def scatter_stage(box, refs, group, xs):
    masks, smasks, inverse, sinverse = refs["mask"], refs["smask"], refs["inv"], refs["sinv"]
    lane = lane_index()

    def step(t, _):
        r = t * 8 + TOP - HALO
        parts, shats = [], []
        for f in group:
            part, totals = strip_scatter(box, smasks, refs["sw"].at[f], r)
            shat = [total * sinverse[k, pl.ds(r, 8), :] for k, total in enumerate(totals)]
            parts.append(part)
            shats.append(shat)
            for dx in (-1, 0, 1):
                for dz in (-1, 0, 1):
                    shifted = roll_groups(roll_groups(shat, -GROUP * dx), -dz)
                    for k in range(box.tiles):
                        refs["shat"][f, 3 * (dx + 1) + dz + 1, k, pl.ds(r, 8), :] = shifted[k]
        for part_xs in chunks(xs):
            totals = main_scatter(box, masks, [refs["w"].at[f] for f in group], part_xs, r, parts)
            for g, f in enumerate(group):
                for i, x in enumerate(part_xs):
                    hat = totals[g][i] * inverse[x, pl.ds(r, 8), :]
                    refs["hat"][f, 1, x, pl.ds(r, 8), :] = hat
                    refs["hat"][f, 0, x, pl.ds(r, 8), :] = jnp.where(
                        lane == 0, from_strip(shats[g], x, LAST, 0), roll(hat, 1)
                    )
                    refs["hat"][f, 2, x, pl.ds(r, 8), :] = jnp.where(
                        lane == LANES - 1, from_strip(shats[g], x, NEXT, LANES - 1), roll(hat, -1)
                    )
        return 0

    lax.fori_loop(0, box.steps, step, 0)


def gather_stage(box, refs, group, xs, out):
    masks, smasks = refs["mask"], refs["smask"]
    first = TOP - HALO if out is None else TOP
    steps = box.steps if out is None else box.sy // 8

    def step(t, _):
        r = t * 8 + first
        for f in group if out is None else ():
            sums = [None] * box.tiles
            for dx, dy, dz in offsets():
                for k in range(box.tiles):
                    piece = refs["shat"][f, 3 * (dx + 1) + dz + 1, k, pl.ds(r + dy, 8), :]
                    if (dx, dy, dz) != (0, 0, 0):
                        piece = piece * smasks[slot_of(dx, dy, dz), k, pl.ds(r, 8), :]
                    sums[k] = add(sums[k], piece)
            for k in range(box.tiles):
                refs["sw"][f, k, pl.ds(r, 8), :] = sums[k] * refs["sscale"][k, pl.ds(r, 8), :]
        for part_xs in chunks(xs):
            sums = main_gather(box, masks, [refs["hat"].at[f] for f in group], part_xs, r)
            for g, f in enumerate(group):
                for i, x in enumerate(part_xs):
                    if out is None:
                        refs["w"][f, x, pl.ds(r, 8), :] = sums[g][i] * refs["scale"][x, pl.ds(r, 8), :]
                    else:
                        out[f, x, pl.ds(t * 8, 8), :] = sums[g][i] * refs["icount"][x, pl.ds(r, 8), :]
        return 0

    lax.fori_loop(0, steps, step, 0)


def masks_stage(box, refs):
    def one(active, kappa, mask, inv_count, scale, index, r):
        count = None
        for dx, dy, dz in offsets():
            if (dx, dy, dz) == (0, 0, 0):
                continue
            bit = jnp.bitwise_and(jnp.right_shift(active, bit_of(dx, dy, dz)), 1).astype(jnp.float32)
            mask[slot_of(dx, dy, dz), index, pl.ds(r, 8), :] = bit
            count = add(count, bit)
        inverse = 1.0 / (count + 1.0)
        if inv_count is not None:
            inv_count[index, pl.ds(r, 8), :] = inverse
        scale[index, pl.ds(r, 8), :] = inverse * kappa

    def step(t, _):
        r = t * 8 + TOP - HALO
        for k in range(box.tiles):
            kappa = refs["skappa"][k, pl.ds(r, 8), :]
            one(refs["sactive"][k, pl.ds(r, 8), :], kappa, refs["smask"], None, refs["sscale"], k, r)
        for x in range(box.planes):
            kappa = refs["kappa"][x, pl.ds(r, 8), :]
            one(refs["active"][x, pl.ds(r, 8), :], kappa, refs["mask"], refs["icount"], refs["scale"], x, r)
        return 0

    lax.fori_loop(0, box.steps, step, 0)


def volume_stage(box, refs, xs):
    def step(t, _):
        r = t * 8 + TOP - HALO
        part, totals = strip_scatter(box, refs["smask"], refs["skappa"], r)
        for k in range(box.tiles):
            refs["sinv"][k, pl.ds(r, 8), :] = 1.0 / totals[k]
        for part_xs in chunks(xs):
            totals = main_scatter(box, refs["mask"], [refs["kappa"]], part_xs, r, [part])
            for i, x in enumerate(part_xs):
                refs["inv"][x, pl.ds(r, 8), :] = 1.0 / totals[0][i]
        return 0

    lax.fori_loop(0, box.steps, step, 0)


GEOMETRY = ("mask", "smask", "inv", "sinv", "icount", "scale", "sscale", "kappa", "skappa")


def geometry_shapes(box):
    p, k, r = box.planes, box.tiles, box.rows
    shapes = [(26, p), (26, k), (p,), (k,), (p,), (p,), (k,), (p,), (k,)]
    return [pltpu.VMEM((*shape, r, LANES), jnp.float32) for shape in shapes]


class Edges:
    def __init__(self, box, edges, zbuf):
        self.box, self.edges, self.zbuf = box, edges, zbuf
        sy, main = box.sy, (box.count + 3) * box.sx * HALO
        self.ylow, self.yhigh, self.corner = 2 * sy, 2 * sy + main + 2 * HALO, main
        self.own, self.before, self.after = pl.ds(TOP, sy), pl.ds(TOP - HALO, HALO), pl.ds(TOP + sy, HALO)

    def columns(self):
        for b, edge in enumerate(self.edges):
            for side in range(2):
                corner = self.corner + side * HALO
                self.zbuf[side, b, self.own, :] = edge[pl.ds(side * self.box.sy, self.box.sy), :]
                self.zbuf[side, b, self.before, :] = edge[pl.ds(self.ylow + corner, HALO), :]
                self.zbuf[side, b, self.after, :] = edge[pl.ds(self.yhigh + corner, HALO), :]

    def rows(self, target, a, x):
        b, p = divmod(x, self.box.sx)
        row = (a * self.box.sx + p) * HALO
        target[x, self.before, :] = self.edges[b][pl.ds(self.ylow + row, HALO), :]
        target[x, self.after, :] = self.edges[b][pl.ds(self.yhigh + row, HALO), :]

    def strips(self, a, main, strip):
        def side_of(side):
            def get(b, r):
                tile = self.zbuf[side, b, pl.ds(r, 8), :]
                return [(tile, (a * self.box.sx + p) * HALO) for p in range(self.box.sx)]

            return get

        fill(self.box, lambda x, r: main[x, pl.ds(r, 8), :], side_of(0), side_of(1), strip)


def geometry_kernel(box, *refs):
    nb = box.blocks
    ints, edge_refs, refs = refs[:nb], refs[nb : 2 * nb], refs[2 * nb :]
    out, refs = dict(zip(GEOMETRY, refs)), refs[len(GEOMETRY) :]
    active, sactive, half, shalf, zbuf = refs
    edges = Edges(box, edge_refs, zbuf)
    edges.columns()
    for x in range(box.planes):
        b, p = divmod(x, box.sx)
        out["kappa"][x, edges.own, :] = ints[b][0, p].astype(jnp.float32)
        member = ints[b][1, p]
        half[0, x, edges.own, :] = jnp.bitwise_and(member, 2**LOW_BITS - 1).astype(jnp.float32)
        half[1, x, edges.own, :] = jnp.right_shift(member, LOW_BITS).astype(jnp.float32)
        edges.rows(out["kappa"], box.count, x)
        edges.rows(half.at[0], box.count + 1, x)
        edges.rows(half.at[1], box.count + 2, x)
    edges.strips(box.count, out["kappa"], out["skappa"])
    for i in range(2):
        edges.strips(box.count + 1 + i, half.at[i], shalf.at[i])

    def convert(t, _):
        rows = pl.ds(t * 8 + TOP - HALO, 8)
        for full, kappa, bits, n in (
            (half, out["kappa"], active, box.planes),
            (shalf, out["skappa"], sactive, box.tiles),
        ):
            for x in range(n):
                kappa[x, rows, :] = kappa[x, rows, :] * 2.0**-20
                low, high = full[0, x, rows, :].astype(jnp.int32), full[1, x, rows, :].astype(jnp.int32)
                bits[x, rows, :] = low + high * 2**LOW_BITS
        return 0

    lax.fori_loop(0, box.steps, convert, 0)
    out.update(active=active, sactive=sactive)
    masks_stage(box, out)
    volume_stage(box, out, box.near(HALO - 1))


def geometry(box, ints, edges):
    p, k, r = box.planes, box.tiles, box.rows
    f32 = jnp.float32
    return pl.pallas_call(
        functools.partial(geometry_kernel, box),
        out_shape=geometry_shapes(box),
        in_specs=[VMEM] * (2 * box.blocks),
        out_specs=[VMEM] * len(GEOMETRY),
        scratch_shapes=[
            pltpu.VMEM((p, r, LANES), jnp.int32),
            pltpu.VMEM((k, r, LANES), jnp.int32),
            pltpu.VMEM((2, p, r, LANES), f32),
            pltpu.VMEM((2, k, r, LANES), f32),
            pltpu.VMEM((2, box.blocks, r, LANES), f32),
        ],
        compiler_params=params(20),
        name="geometry",
    )(*ints, *edges)


WORK = ("w", "sw", "hat", "shat")


def fields_kernel(box, group, aliased, *refs):
    nb, n = box.blocks, len(group)
    fields, edge_refs, refs = refs[:nb], refs[nb : 2 * nb], refs[2 * nb :]
    known, refs = dict(zip(GEOMETRY, refs)), refs[len(GEOMETRY) + aliased :]
    merged, refs = refs[0], refs[1:]
    known.update(zip(WORK, refs))
    zbuf, result, done = refs[len(WORK) :]
    edges = Edges(box, edge_refs, zbuf)
    edges.columns()
    for i, f in enumerate(group):
        w, sw = known["w"].at[i], known["sw"].at[i]
        for x in range(box.planes):
            b, p = divmod(x, box.sx)
            w[x, edges.own, :] = fields[b][f if b == 0 else i, p]
            edges.rows(w, f, x)
        edges.strips(f, w, sw)

    def weigh(t, _):
        rows = pl.ds(t * 8 + TOP - HALO, 8)
        for i in range(n):
            for x in range(box.planes):
                known["w"][i, x, rows, :] = known["w"][i, x, rows, :] * known["kappa"][x, rows, :]
            for k in range(box.tiles):
                known["sw"][i, k, rows, :] = known["sw"][i, k, rows, :] * known["skappa"][k, rows, :]
        return 0

    lax.fori_loop(0, box.steps, weigh, 0)
    inner = list(range(n))
    for step in range(PASSES):
        reach = HALO - 1 - 2 * step
        scatter_stage(box, known, inner, box.near(reach))
        gather_stage(box, known, inner, box.near(reach - 1), None if step < PASSES - 1 else result)
    copy = pltpu.make_async_copy(result, merged.at[pl.ds(group[0], n)], done)
    copy.start()
    copy.wait()


def merge(box, group, fields, edges, known, merged):
    p, k, r, n = box.planes, box.tiles, box.rows, len(group)
    f32 = jnp.float32
    shape = fields[0].shape
    aliased = merged is not None
    operands = [*fields, *edges, *known]
    specs = [VMEM] * len(operands)
    return pl.pallas_call(
        functools.partial(fields_kernel, box, group, aliased),
        out_shape=jax.ShapeDtypeStruct(shape, f32),
        in_specs=specs + [ANY] * aliased,
        out_specs=ANY,
        scratch_shapes=[
            pltpu.VMEM((n, p, r, LANES), f32),
            pltpu.VMEM((n, k, r, LANES), f32),
            pltpu.VMEM((n, 3, p, r, LANES), f32),
            pltpu.VMEM((n, 9, k, r, LANES), f32),
            pltpu.VMEM((2, box.blocks, r, LANES), f32),
            pltpu.VMEM((n, *shape[1:]), f32),
            pltpu.SemaphoreType.DMA(()),
        ],
        input_output_aliases={len(operands): 0} if aliased else {},
        compiler_params=params(16),
        name="merge",
    )(*operands, *([merged] if aliased else []))


def body(fields, volume_code, cut_flag, member_bits):
    count, sx, sy, _ = fields.shape
    size = lax.axis_size("gx")

    def from_x(value):
        if size == 1:
            return []
        if size == 2:
            return [lax.ppermute(value, "gx", ring("gx", 1))]
        return [lax.ppermute(value, "gx", ring("gx", -1)), lax.ppermute(value, "gx", ring("gx", 1))]

    ints, zlo, zhi, ylo, yhi = pack(fields, volume_code, cut_flag, member_bits)
    low = lax.ppermute(zhi, "gz", ring("gz", 1))
    high = lax.ppermute(zlo, "gz", ring("gz", -1))
    all_ints = [ints] + from_x(ints)
    box = Box(count, sx, sy, len(all_ints))
    groups = chunks(list(range(count)), 2)
    shared = [from_x(fields[groups[0][0] : groups[0][-1] + 1])]
    ylo, yhi = add_corners(low, high, ylo, yhi)
    before = lax.ppermute(yhi, "gy", ring("gy", 1))
    after = lax.ppermute(ylo, "gy", ring("gy", -1))
    edge = join(low, high, before, after)
    all_edges = [edge] + from_x(edge)
    for group in groups[1:]:
        shared.append(from_x(fields[group[0] : group[-1] + 1]))
    known = geometry(box, all_ints, all_edges)
    merged = None
    for group, others in zip(groups, shared):
        merged = merge(box, group, [fields] + others, all_edges, known, merged)
    return merged


def solution(mesh):
    in_specs = (
        P(None, "gx", "gy", "gz"),
        P("gx", "gy", "gz"),
        P("gx", "gy", "gz"),
        P("gx", "gy", "gz"),
    )
    out_specs = P(None, "gx", "gy", "gz")
    return jax.shard_map(body, mesh=mesh, in_specs=in_specs, out_specs=out_specs, check_vma=False)
```

```python
import functools

import jax
import jax.numpy as jnp
from jax import lax
from jax.experimental import pallas as pl
from jax.experimental.pallas import tpu as pltpu
from jax.sharding import PartitionSpec as P


PASSES = 2
HALO = 2 * PASSES
LANES = 128
GROUP = 16
TOP = 16
LOW_BITS = 14

VMEM = pl.BlockSpec(memory_space=pltpu.VMEM)
ANY = pl.BlockSpec(memory_space=pltpu.HBM)


def params(mib):
    return pltpu.CompilerParams(vmem_limit_bytes=int(mib * 2**20))


def offsets():
    return [(dx, dy, dz) for dx in (-1, 0, 1) for dy in (-1, 0, 1) for dz in (-1, 0, 1)]


def bit_of(dx, dy, dz):
    return 9 * (dx + 1) + 3 * (dy + 1) + (dz + 1)


def slot_of(dx, dy, dz):
    index = bit_of(dx, dy, dz)
    return index if index < 13 else index - 1


def roll(value, shift):
    shift = shift % LANES
    return value if shift == 0 else pltpu.roll(value, shift, 1)


def ring(axis, step):
    count = lax.axis_size(axis)
    return [(i, (i + step) % count) for i in range(count)]


def pack_kernel(fields, code, flag, bits, *refs):
    pairs, refs = refs[:-9], refs[-9:]
    ints, zlo, zhi, ylo, yhi, flag_v, bits_v, sems, field_sems = refs
    count, sx, sy, _ = fields.shape
    copies = [
        pltpu.make_async_copy(flag, flag_v, sems.at[0]),
        pltpu.make_async_copy(bits, bits_v, sems.at[1]),
        pltpu.make_async_copy(code, ints.at[0], sems.at[2]),
    ]
    loads, first = [], 0
    for i, pair in enumerate(pairs):
        loads.append(pltpu.make_async_copy(fields.at[pl.ds(first, pair.shape[0])], pair, field_sems.at[i]))
        first += pair.shape[0]
    for copy in copies + loads:
        copy.start()
    lane = lax.broadcasted_iota(jnp.int32, (sy, LANES), 1)
    sides = [jnp.zeros((sy, LANES), jnp.float32)] * 2

    def place(a, p, plane, sides):
        row = (a * sx + p) * HALO
        ylo[pl.ds(row, HALO), :] = plane[:HALO]
        yhi[pl.ds(row, HALO), :] = plane[sy - HALO :]
        here = (lane >= row) & (lane < row + HALO)
        return [
            jnp.where(here, roll(plane, row), sides[0]),
            jnp.where(here, roll(plane, row + HALO), sides[1]),
        ]

    for copy in copies:
        copy.wait()
    for p in range(sx):
        active = bits_v[p] * flag_v[p]
        ints[1, p] = active
        low = jnp.bitwise_and(active, 2**LOW_BITS - 1).astype(jnp.float32)
        high = jnp.right_shift(active, LOW_BITS).astype(jnp.float32)
        for i, plane in enumerate((ints[0, p].astype(jnp.float32), low, high)):
            sides = place(count + i, p, plane, sides)
    f = 0
    for pair, load in zip(pairs, loads):
        load.wait()
        for i in range(pair.shape[0]):
            for p in range(sx):
                sides = place(f, p, pair[i, p], sides)
            f += 1
    zlo[...], zhi[...] = sides


def pack(groups, fields, code, flag, bits):
    count, sx, sy, sz = fields.shape
    rows = (count + 3) * sx * HALO + 2 * HALO
    f32 = jnp.float32
    pairs = [pltpu.VMEM((len(group), sx, sy, sz), f32) for group in groups]
    outs = pl.pallas_call(
        pack_kernel,
        out_shape=(
            *pairs,
            pltpu.VMEM((2, sx, sy, sz), jnp.int32),
            pltpu.VMEM((sy, LANES), f32),
            pltpu.VMEM((sy, LANES), f32),
            pltpu.VMEM((rows, LANES), f32),
            pltpu.VMEM((rows, LANES), f32),
        ),
        in_specs=[ANY] * 4,
        out_specs=(VMEM,) * (len(pairs) + 5),
        scratch_shapes=[
            pltpu.VMEM((sx, sy, sz), jnp.int32),
            pltpu.VMEM((sx, sy, sz), jnp.int32),
            pltpu.SemaphoreType.DMA((3,)),
            pltpu.SemaphoreType.DMA((len(pairs),)),
        ],
        compiler_params=params(62.9),
        name="pack",
    )(fields, code, flag, bits)
    return outs[: len(pairs)], *outs[len(pairs) :]


def corners_kernel(sy, low, high, ylo_in, yhi_in, ylo, yhi):
    first = ylo.shape[0] - 2 * HALO
    for side, column in enumerate((low, high)):
        rows = pl.ds(first + side * HALO, HALO)
        ylo[rows, :] = column[:HALO]
        yhi[rows, :] = column[sy - HALO :]


def add_corners(low, high, ylo, yhi):
    shape = jax.ShapeDtypeStruct(ylo.shape, ylo.dtype)
    return pl.pallas_call(
        functools.partial(corners_kernel, low.shape[0]),
        out_shape=(shape, shape),
        in_specs=[VMEM] * 4,
        out_specs=(VMEM, VMEM),
        input_output_aliases={2: 0, 3: 1},
        compiler_params=params(2),
        name="corners",
    )(low, high, ylo, yhi)


def join_kernel(*refs):
    out, row = refs[-1], 0
    for ref in refs[:-1]:
        out[pl.ds(row, ref.shape[0]), :] = ref[...]
        row += ref.shape[0]


def join(*pieces):
    rows = sum(piece.shape[0] for piece in pieces)
    return pl.pallas_call(
        join_kernel,
        out_shape=jax.ShapeDtypeStruct((rows, LANES), jnp.float32),
        in_specs=[VMEM] * len(pieces),
        out_specs=VMEM,
        compiler_params=params(2),
        name="join",
    )(*pieces)


class Box:
    def __init__(self, count, sx, sy, blocks):
        self.count, self.sx, self.sy, self.blocks = count, sx, sy, blocks
        self.planes = sx * blocks
        self.tiles = -(-self.planes * GROUP // LANES)
        self.steps = -(-(sy + 2 * HALO) // 8)
        self.rows = TOP + sy + 8

    def near(self, reach):
        return sorted({x % self.planes for x in range(-reach, self.sx + reach)})

    def first(self, t):
        return t * 8 + TOP - HALO


def lane_index():
    return lax.broadcasted_iota(jnp.int32, (8, LANES), 1)


def roll_groups(values, shift):
    count = len(values)
    rolled = [roll(v, shift) for v in values]
    if count == 1 or shift == 0:
        return rolled
    lane = lane_index()
    if shift > 0:
        return [jnp.where(lane < shift, rolled[(k - 1) % count], rolled[k]) for k in range(count)]
    return [jnp.where(lane >= LANES + shift, rolled[(k + 1) % count], rolled[k]) for k in range(count)]


def add(left, right):
    return right if left is None else left + right


def from_strip(tiles, x, column, lane):
    tile, first = divmod(x * GROUP + column, LANES)
    return roll(tiles[tile], lane - first)


LAST = HALO - 1
NEXT = 3 * HALO


def version(dx, dz):
    return 3 * (dx + 1) + dz + 1


def spread_strip(box, tiles, target, r):
    for dx in (-1, 0, 1):
        for dz in (-1, 0, 1):
            shifted = roll_groups(tiles, -GROUP * dx - dz)
            for k in range(box.tiles):
                target[version(dx, dz), k, pl.ds(r, 8), :] = shifted[k]


def spread_plane(value, tiles, target, x, r):
    lane = lane_index()
    before, after = from_strip(tiles, x, LAST, 0), from_strip(tiles, x, NEXT, LANES - 1)
    target[0, x, pl.ds(r, 8), :] = jnp.where(lane == 0, before, roll(value, 1))
    target[2, x, pl.ds(r, 8), :] = jnp.where(lane == LANES - 1, after, roll(value, -1))


def center_strip(box, source, r):
    return [source[version(0, 0), k, pl.ds(r, 8), :] for k in range(box.tiles)]


def masked_strip(box, masks, sources, sign, r):
    sums = [[None] * box.tiles for _ in sources]
    for dx, dy, dz in offsets():
        for k in range(box.tiles):
            mask = None
            if (dx, dy, dz) != (0, 0, 0):
                mask = masks[slot_of(dx, dy, dz), k, pl.ds(r, 8), :]
            for f, source in enumerate(sources):
                piece = source[version(sign * dx, sign * dz), k, pl.ds(r + sign * dy, 8), :]
                sums[f][k] = add(sums[f][k], piece if mask is None else piece * mask)
    return sums


def masked_planes(box, masks, sources, sign, xs, r):
    sums = [{x: None for x in xs} for _ in sources]
    for dy in (-1, 0, 1):
        for dz in (-1, 0, 1):
            for at in range(box.planes):
                targets = [((at - sign * dx) % box.planes, dx) for dx in (-1, 0, 1)]
                targets = [(x, dx) for x, dx in targets if x in xs]
                if not targets:
                    continue
                cells = [source[sign * dz + 1, at, pl.ds(r + sign * dy, 8), :] for source in sources]
                for x, dx in targets:
                    mask = None
                    if (dx, dy, dz) != (0, 0, 0):
                        mask = masks[slot_of(dx, dy, dz), x, pl.ds(r, 8), :]
                    for f, cell in enumerate(cells):
                        sums[f][x] = add(sums[f][x], cell if mask is None else cell * mask)
    return sums


def stage(box, masks, smasks, scale, sscale, sources, ssources, targets, stargets, sign, xs):
    def spread(r):
        for target, starget in zip(targets, stargets):
            tiles = center_strip(box, starget, r)
            for x in xs:
                spread_plane(target[1, x, pl.ds(r, 8), :], tiles, target, x, r)

    def step(t, _):
        r = box.first(t)
        sums = masked_strip(box, smasks, ssources, sign, r)
        for f, starget in enumerate(stargets):
            tiles = [total * sscale[k, pl.ds(r, 8), :] for k, total in enumerate(sums[f])]
            spread_strip(box, tiles, starget, r)
        spread(r - 8)
        sums = masked_planes(box, masks, sources, sign, xs, r)
        for f, target in enumerate(targets):
            for x in xs:
                target[1, x, pl.ds(r, 8), :] = sums[f][x] * scale[x, pl.ds(r, 8), :]
        return 0

    lax.fori_loop(0, box.steps, step, 0)
    spread(box.first(box.steps - 1))


def bit_value(active, dx, dy, dz):
    return jnp.bitwise_and(jnp.right_shift(active, bit_of(dx, dy, dz)), 1).astype(jnp.float32)


GEOMETRY = ("own", "sown", "from", "sfrom", "inv", "sinv", "icount", "scale", "sscale", "kappa", "skappa")


def geometry_shapes(box):
    p, k, r = box.planes, box.tiles, box.rows
    shapes = [(26, p), (26, k), (26, p), (26, k), (p,), (k,), (p,), (p,), (k,), (p,), (k,)]
    return [pltpu.VMEM((*shape, r, LANES), jnp.float32) for shape in shapes]


class Edges:
    def __init__(self, box, edges):
        self.box, self.edges = box, edges
        sy, main = box.sy, (box.count + 3) * box.sx * HALO
        self.ylow, self.yhigh, self.corner = 2 * sy, 2 * sy + main + 2 * HALO, main
        self.own, self.before, self.after = pl.ds(TOP, sy), pl.ds(TOP - HALO, HALO), pl.ds(TOP + sy, HALO)

    def columns(self, zbuf):
        for b, edge in enumerate(self.edges):
            for side in range(2):
                corner = self.corner + side * HALO
                zbuf[side, b, self.own, :] = edge[pl.ds(side * self.box.sy, self.box.sy), :]
                zbuf[side, b, self.before, :] = edge[pl.ds(self.ylow + corner, HALO), :]
                zbuf[side, b, self.after, :] = edge[pl.ds(self.yhigh + corner, HALO), :]

    def row(self, a, x):
        return (a * self.box.sx + x % self.box.sx) * HALO

    def rows(self, a, x):
        edge = self.edges[x // self.box.sx]
        row = self.row(a, x)
        return edge[pl.ds(self.ylow + row, HALO), :], edge[pl.ds(self.yhigh + row, HALO), :]

    def strip(self, main, low_of, high_of, a, r):
        lane = lane_index()
        out = [None] * self.box.tiles
        for b in range(self.box.blocks):
            low, high = low_of(b, r), high_of(b, r)
            for p in range(self.box.sx):
                x = b * self.box.sx + p
                tile, first = divmod(x * GROUP, LANES)
                plane = main[x, pl.ds(r, 8), :]
                column = self.row(a, x)
                for c, (data, at) in enumerate(((low, column), (plane, 0), (plane, LANES - HALO), (high, column))):
                    to = first + c * HALO
                    moved = roll(data, to - at)
                    out[tile] = moved if out[tile] is None else jnp.where(lane >= to, moved, out[tile])
        return out


def geometry_kernel(box, *refs):
    nb = box.blocks
    ints, edge_refs, refs = refs[:nb], refs[nb : 2 * nb], refs[2 * nb :]
    out, refs = dict(zip(GEOMETRY, refs)), refs[len(GEOMETRY) :]
    active, sactive, kappa, skappa, zbuf = refs
    edges = Edges(box, edge_refs)
    edges.columns(zbuf)
    unit = 2.0**-20

    def whole(low, high):
        return low.astype(jnp.int32) + high.astype(jnp.int32) * 2**LOW_BITS

    for x in range(box.planes):
        b, p = divmod(x, box.sx)
        kappa[1, x, edges.own, :] = ints[b][0, p].astype(jnp.float32) * unit
        active[1, x, edges.own, :] = ints[b][1, p]
        for here, rows in enumerate((edges.before, edges.after)):
            code, low, high = [edges.rows(box.count + i, x)[here] for i in range(3)]
            kappa[1, x, rows, :] = code * unit
            active[1, x, rows, :] = whole(low, high)

    def code_of(side):
        return lambda b, r: zbuf[side, b, pl.ds(r, 8), :] * unit

    def bits_of(side):
        def get(b, r):
            tile = zbuf[side, b, pl.ds(r, 8), :]
            return whole(tile, roll(tile, -box.sx * HALO))

        return get

    for t in range(box.steps):
        r = box.first(t)
        for main, strip, halo, a in ((kappa, skappa, code_of, box.count), (active, sactive, bits_of, box.count + 1)):
            tiles = edges.strip(main.at[1], halo(0), halo(1), a, r)
            spread_strip(box, tiles, strip, r)

    def spread(t, _):
        r = box.first(t)
        for main, strip in ((kappa, skappa), (active, sactive)):
            tiles = center_strip(box, strip, r)
            for x in range(box.planes):
                spread_plane(main[1, x, pl.ds(r, 8), :], tiles, main, x, r)
        return 0

    lax.fori_loop(0, box.steps, spread, 0, unroll=3)

    def masks(t, _):
        r = box.first(t)
        rows = pl.ds(r, 8)
        for n, center, source, values, own, back, icount, scale, plain in (
            (box.planes, 1, active, kappa, "own", "from", "icount", "scale", "kappa"),
            (box.tiles, version(0, 0), sactive, skappa, "sown", "sfrom", None, "sscale", "skappa"),
        ):
            for x in range(n):
                here, total = source[center, x, rows, :], None
                for dx, dy, dz in offsets():
                    if (dx, dy, dz) == (0, 0, 0):
                        continue
                    bit = bit_value(here, dx, dy, dz)
                    out[own][slot_of(dx, dy, dz), x, rows, :] = bit
                    total = add(total, bit)
                    if center == 1:
                        there = source[1 - dz, (x - dx) % box.planes, pl.ds(r - dy, 8), :]
                    else:
                        there = source[version(-dx, -dz), x, pl.ds(r - dy, 8), :]
                    out[back][slot_of(dx, dy, dz), x, rows, :] = bit_value(there, dx, dy, dz)
                inverse = 1.0 / (total + 1.0)
                value = values[center, x, rows, :]
                out[plain][x, rows, :] = value
                out[scale][x, rows, :] = inverse * value
                if icount is not None:
                    out[icount][x, rows, :] = inverse
        return 0

    lax.fori_loop(0, box.steps, masks, 0)

    def volumes(t, _):
        r = box.first(t)
        totals = masked_strip(box, out["sfrom"], [skappa], -1, r)[0]
        for k, total in enumerate(totals):
            out["sinv"][k, pl.ds(r, 8), :] = 1.0 / total
        totals = masked_planes(box, out["from"], [kappa], -1, box.near(HALO - 1), r)[0]
        for x, total in totals.items():
            out["inv"][x, pl.ds(r, 8), :] = 1.0 / total
        return 0

    lax.fori_loop(0, box.steps, volumes, 0)


def geometry(box, ints, edges):
    p, k, r = box.planes, box.tiles, box.rows
    f32 = jnp.float32
    return pl.pallas_call(
        functools.partial(geometry_kernel, box),
        out_shape=geometry_shapes(box),
        in_specs=[VMEM] * (2 * box.blocks),
        out_specs=[VMEM] * len(GEOMETRY),
        scratch_shapes=[
            pltpu.VMEM((3, p, r, LANES), jnp.int32),
            pltpu.VMEM((9, k, r, LANES), jnp.int32),
            pltpu.VMEM((3, p, r, LANES), f32),
            pltpu.VMEM((9, k, r, LANES), f32),
            pltpu.VMEM((2, box.blocks, r, LANES), f32),
        ],
        compiler_params=params(8),
        name="geometry",
    )(*ints, *edges)


def fields_kernel(box, group, aliased, *refs):
    nb, n = box.blocks, len(group)
    fields, edge_refs, refs = refs[:nb], refs[nb : 2 * nb], refs[2 * nb :]
    known, refs = dict(zip(GEOMETRY, refs)), refs[len(GEOMETRY) + aliased :]
    merged, w, sw, hat, shat, zbuf, result, done = refs
    edges = Edges(box, edge_refs)
    edges.columns(zbuf)
    for i, f in enumerate(group):
        for x in range(box.planes):
            b, p = divmod(x, box.sx)
            before, after = edges.rows(f, x)
            w[i, 1, x, edges.own, :] = fields[b][i, p]
            w[i, 1, x, edges.before, :] = before
            w[i, 1, x, edges.after, :] = after

    def halo(side):
        return lambda b, r: zbuf[side, b, pl.ds(r, 8), :]

    def weigh(t, _):
        rows = pl.ds(box.first(t), 8)
        for i, f in enumerate(group):
            tiles = edges.strip(w.at[i, 1], halo(0), halo(1), f, box.first(t))
            tiles = [tile * known["skappa"][k, rows, :] for k, tile in enumerate(tiles)]
            spread_strip(box, tiles, sw.at[i], box.first(t))
            for x in range(box.planes):
                value = w[i, 1, x, rows, :] * known["kappa"][x, rows, :]
                w[i, 1, x, rows, :] = value
                spread_plane(value, tiles, w.at[i], x, box.first(t))
        return 0

    lax.fori_loop(0, box.steps, weigh, 0, unroll=3)

    def each(ref):
        return [ref.at[i] for i in range(n)]

    copy = pltpu.make_async_copy(result, merged.at[pl.ds(group[0], n)], done)
    for step in range(PASSES):
        reach = HALO - 1 - 2 * step
        stage(box, known["from"], known["sfrom"], known["inv"], known["sinv"], each(w), each(sw), each(hat), each(shat), -1, box.near(reach))
        if step < PASSES - 1:
            stage(box, known["own"], known["sown"], known["scale"], known["sscale"], each(hat), each(shat), each(w), each(sw), 1, box.near(reach - 1))

    def last(t, _):
        r = TOP + t * 8
        sums = masked_planes(box, known["own"], each(hat), 1, box.near(0), r)
        rows = pl.ds(t * 8, 8)
        for i in range(n):
            for x in range(box.sx):
                result[i, x, rows, :] = sums[i][x] * known["icount"][x, pl.ds(r, 8), :]
        pltpu.make_async_copy(result.at[:, :, rows], merged.at[pl.ds(group[0], n), :, rows], done).start()
        return 0

    lax.fori_loop(0, box.sy // 8, last, 0)
    copy.wait()


def merge(box, group, fields, edges, known, merged):
    p, k, r, n = box.planes, box.tiles, box.rows, len(group)
    f32 = jnp.float32
    sizes = fields[0].shape[1:]
    aliased = merged is not None
    operands = [*fields, *edges, *known]
    specs = [VMEM] * len(operands)
    return pl.pallas_call(
        functools.partial(fields_kernel, box, group, aliased),
        out_shape=jax.ShapeDtypeStruct((box.count, *sizes), f32),
        in_specs=specs + [ANY] * aliased,
        out_specs=ANY,
        scratch_shapes=[
            pltpu.VMEM((n, 3, p, r, LANES), f32),
            pltpu.VMEM((n, 9, k, r, LANES), f32),
            pltpu.VMEM((n, 3, p, r, LANES), f32),
            pltpu.VMEM((n, 9, k, r, LANES), f32),
            pltpu.VMEM((2, box.blocks, r, LANES), f32),
            pltpu.VMEM((n, *sizes), f32),
            pltpu.SemaphoreType.DMA(()),
        ],
        input_output_aliases={len(operands): 0} if aliased else {},
        compiler_params=params(14),
        name="merge",
    )(*operands, *([merged] if aliased else []))


def body(fields, volume_code, cut_flag, member_bits):
    count, sx, sy, _ = fields.shape
    size = lax.axis_size("gx")

    def from_x(value):
        if size == 1:
            return []
        if size == 2:
            return [lax.ppermute(value, "gx", ring("gx", 1))]
        return [lax.ppermute(value, "gx", ring("gx", -1)), lax.ppermute(value, "gx", ring("gx", 1))]

    groups = [list(range(count))[i : i + 2] for i in range(0, count, 2)]
    pairs, ints, zlo, zhi, ylo, yhi = pack(groups, fields, volume_code, cut_flag, member_bits)
    all_ints = [ints] + from_x(ints)
    low = lax.ppermute(zhi, "gz", ring("gz", 1))
    high = lax.ppermute(zlo, "gz", ring("gz", -1))
    box = Box(count, sx, sy, len(all_ints))
    shared = [[pairs[0]] + from_x(pairs[0])]
    ylo, yhi = add_corners(low, high, ylo, yhi)
    before = lax.ppermute(yhi, "gy", ring("gy", 1))
    after = lax.ppermute(ylo, "gy", ring("gy", -1))
    edge = join(low, high, before, after)
    all_edges = [edge] + from_x(edge)
    for pair in pairs[1:]:
        shared.append([pair] + from_x(pair))
    known = geometry(box, all_ints, all_edges)
    merged = None
    for group, blocks in zip(groups, shared):
        merged = merge(box, group, blocks, all_edges, known, merged)
    return merged


def solution(mesh):
    in_specs = (
        P(None, "gx", "gy", "gz"),
        P("gx", "gy", "gz"),
        P("gx", "gy", "gz"),
        P("gx", "gy", "gz"),
    )
    out_specs = P(None, "gx", "gy", "gz")
    return jax.shard_map(body, mesh=mesh, in_specs=in_specs, out_specs=out_specs, check_vma=False)
```
